32 devices in a mesh: aux: 4 (over x, core), ao: 8 (over z, y).
Axes of the slice: x: 2, y: 2, z: 4, core: 2. Of those that a mesh axis runs over, the one named last changes fastest.
Arguments:
- cholesky: bfloat16 [64, 4096, 4096], P('aux', 'ao'), may hold values from -3.5 to 3.5, as said below
- coeffs: bfloat16 [4096, 128], P('ao'), may hold values from -0.09375 to 0.09375
Outputs:
- integrals: float32 [16384, 16384], P('aux', 'ao')
The draws below stay inside these ranges and needn't reach their ends.
Inputs may be any that keep to these rules, and one draw needn't show every extreme that they name: cholesky[L, mu, nu] = cholesky[L, nu, mu] for every vector L.
All inputs are finite; a program needn't handle non-finite values.
Results may differ from the reference program's by a relative error of at most 0.0091.
Values may be sent and summed in bfloat16 or wider, within the bound.
A program may use at most 192 MiB of HBM per device.

```python
import math
import jax
import jax.numpy as jnp
from jax import lax

NAO = 4096
NACT = 128
NVEC = 64


def draw_cholesky(key, part):
    slab_keys = jax.random.split(jax.random.fold_in(key, 11), NVEC)
    scales = jnp.ones((NVEC, NAO), jnp.float32)

    def one_slab(inputs):
        slab_key, row_scale = inputs
        values = 0.35 * jax.random.normal(slab_key, (NAO, NAO), jnp.float32)
        values = jnp.clip(values, -2.5, 2.5)
        sym = (values + values.T) / math.sqrt(2.0)
        sym = sym * row_scale[:, None] * row_scale[None, :]
        return jnp.clip(sym, -3.5, 3.5).astype(jnp.bfloat16)
    return lax.map(one_slab, (slab_keys, scales))


def steps_of(own_key, dims, cuts, smallest, high):
    loudness = 1.0
    for axis_at, shards_of in cuts:
        heights = jax.random.uniform(jax.random.fold_in(jax.random.fold_in(own_key, 6), axis_at), (shards_of,), jnp.float32, smallest / len(cuts), high / len(cuts))
        loudness = loudness * jnp.repeat(jnp.exp(heights), dims[axis_at] // shards_of).reshape((-1,) + (1,) * (len(dims) - 1 - axis_at))
    return loudness


def scatter_about(rng, extent, spread, bound, shards=(), held_as=jnp.bfloat16):
    drawn = jax.random.normal(rng, extent, jnp.float32) * spread
    if len(shards) > 0:
        drawn = steps_of(rng, extent, shards, -0.22, 0.18) * drawn
    return jnp.clip(drawn, min=-bound, max=bound).astype(held_as)


def setup_inputs(seed: int = 0) -> dict:
    seeds = jax.random.split(jax.random.key(seed), 3)
    cholesky = draw_cholesky(jax.random.fold_in(seeds[2], 71), 0)
    coeffs = scatter_about(seeds[1], (NAO, NACT), NAO ** -0.5, 0.09375, ((0, 8),))
    return {"cholesky": cholesky, "coeffs": coeffs}


def reference(cholesky, coeffs):
    def one_vector(slab):
        half = jnp.dot(slab, coeffs, preferred_element_type=jnp.float32).astype(jnp.bfloat16)
        return jnp.dot(coeffs.T, half, preferred_element_type=jnp.float32).astype(jnp.bfloat16)

    pairs = lax.map(one_vector, cholesky)
    flat_pairs = pairs.reshape(NVEC, NACT * NACT)
    return lax.dot_general(flat_pairs, flat_pairs, (((0,), (0,)), ((), ())), preferred_element_type=jnp.float32)
```

```python
import functools

import jax
import jax.numpy as jnp
from jax import lax
from jax.experimental import pallas as pl
from jax.experimental.pallas import tpu as pltpu
from jax.sharding import PartitionSpec as P

MESH = pl.DeviceIdType.MESH
F32 = jnp.float32
BF16 = jnp.bfloat16


def dot(a, b):
    return jnp.dot(a, b, preferred_element_type=F32)


def pairs_kernel(
    n_aux, n_ao, n_groups,
    chol, c_ref, left, right,
    slabs, basis, ct, ct_lo, ct_hi, u, part, recv1, part2, recv2, mine,
    slab_sem, c_send, c_recv, f_send, f_recv,
    a1_send, a1_recv, a2_send, a2_recv, r_send, r_recv, l_send, l_recv, y_send, y_recv,
):
    a = lax.axis_index("aux")
    o = lax.axis_index("ao")
    nvec, rows, _ = chol.shape
    active = c_ref.shape[1]
    width = active // n_ao
    reach = n_ao // 2
    nz = n_ao // 2
    half = rows // 2
    fine = half % 128 == 0
    quarter = rows // n_aux
    gv = nvec // n_groups
    y = lax.rem(o, 2)
    z = o // 2
    partner = o + 1 - 2 * y
    ratio = n_ao // n_aux
    hr = ratio // 2
    band_of = o // ratio
    qh = lax.rem(o, ratio) // 2
    home = band_of == a

    def share_copy(d):
        mine_rows = pl.ds(pl.multiple_of(a * quarter, quarter), quarter)
        there = pl.ds(pl.multiple_of(d * rows + a * quarter, quarter), quarter)
        return pltpu.make_async_remote_copy(
            src_ref=c_ref.at[mine_rows], dst_ref=basis.at[there],
            send_sem=c_send.at[d - 1], recv_sem=c_recv.at[d - 1],
            device_id=(a, lax.rem(o + n_ao - d, n_ao)), device_id_type=MESH,
        )

    def forward_copy(d, e):
        there = pl.ds(pl.multiple_of(d * rows + a * quarter, quarter), quarter)
        return pltpu.make_async_remote_copy(
            src_ref=basis.at[there], dst_ref=basis.at[there],
            send_sem=f_send.at[d - 1, e - 1], recv_sem=f_recv.at[d - 1, e - 1],
            device_id=(lax.rem(a + e, n_aux), o), device_id_type=MESH,
        )

    for d in range(1, reach + 1):
        share_copy(d).start()

    deep = (reach + 1) * rows

    def start_vector(v, carry):
        for first in range(n_ao):
            @pl.when(o == first)
            def _():
                run = min(reach + 1, n_ao - first) * rows
                pltpu.make_async_copy(
                    chol.at[v, :, pl.ds(first * rows, run)],
                    slabs.at[v, :, pl.ds(0, run)],
                    slab_sem.at[v],
                ).start()
                if run < deep:
                    pltpu.make_async_copy(
                        chol.at[v, :, pl.ds(0, deep - run)],
                        slabs.at[v, :, pl.ds(run, deep - run)],
                        slab_sem.at[v],
                    ).start()
        return carry

    lax.fori_loop(0, nvec, start_vector, 0)

    basis[pl.ds(0, rows), :] = c_ref[...]
    c_t = c_ref[...].astype(F32).T
    first = lax.broadcasted_iota(jnp.int32, c_t.shape, 1) < (half if fine else 0)
    ct[...] = c_t.astype(BF16)
    ct_lo[...] = jnp.where(first, c_t, 0.5 * c_t).astype(BF16)
    ct_hi[...] = jnp.where(first, 0.5 * c_t, c_t).astype(BF16)

    def contract_rows(v, carry):
        pltpu.make_async_copy(
            chol.at[v, :, pl.ds(0, deep)], slabs.at[v], slab_sem.at[v]
        ).wait()
        out = pl.ds(pl.multiple_of(v * active, active), active)
        if not fine:
            for d in range(reach + 1):
                block = pl.ds(d * rows, rows)
                lhs = ct_lo if d in (0, reach) else ct
                u[out, block] = dot(lhs[...], slabs[v, :, block]).astype(BF16)
            return carry
        lo, hi = pl.ds(0, half), pl.ds(half, half)

        def put(b, value):
            u[out, pl.ds(b * half, half)] = value.astype(BF16)

        put(0, dot(ct_hi[:, lo], slabs[v, lo, pl.ds(0, half)]))
        put(1, dot(ct_lo[...], slabs[v, :, pl.ds(half, half)]))
        for b in range(2, n_ao):
            put(b, dot(ct[...], slabs[v, :, pl.ds(b * half, half)]))
        put(n_ao, dot(ct_hi[...], slabs[v, :, pl.ds(n_ao * half, half)]))
        put(n_ao + 1, dot(ct_lo[:, hi], slabs[v, hi, pl.ds((n_ao + 1) * half, half)]))
        return carry

    def rows_of_group(g):
        lax.fori_loop(g * gv, (g + 1) * gv, contract_rows, 0)

    def a1_copy(g):
        return pltpu.make_async_remote_copy(
            src_ref=part.at[g, 1 - y], dst_ref=recv1.at[g],
            send_sem=a1_send.at[g], recv_sem=a1_recv.at[g],
            device_id=(a, partner), device_id_type=MESH,
        )

    def a2_copy(g, d):
        to = lax.rem(z + d, nz)
        return pltpu.make_async_remote_copy(
            src_ref=part2.at[g, to], dst_ref=recv2.at[g, d - 1],
            send_sem=a2_send.at[g, d - 1], recv_sem=a2_recv.at[g, d - 1],
            device_id=(a, 2 * to + y), device_id_type=MESH,
        )

    def pairs_of_group(g):
        tall = gv * active // 2 if gv % 2 == 0 else gv * active
        x = [dot(u[pl.ds(g * gv * active + r, tall), :], basis[...]) for r in range(0, gv * active, tall)]
        for v in range(gv):
            r = v * active
            one = x[r // tall][r % tall : r % tall + active]
            both = (one + one.T).astype(BF16)
            for q in range(n_ao):
                part[g, q % 2, q // 2, v] = both[q * width : (q + 1) * width]
        a1_copy(g).start()

    def second_level(g):
        a1_copy(g).wait()
        part2[g] = (part[g, y].astype(F32) + recv1[g].astype(F32)).astype(BF16)
        for d in range(1, nz):
            a2_copy(g, d).start()

    def right_copy(g, e):
        return pltpu.make_async_remote_copy(
            src_ref=mine.at[g], dst_ref=right.at[g, a],
            send_sem=r_send.at[g, e - 1], recv_sem=r_recv.at[g, e - 1],
            device_id=(lax.rem(a + e, n_aux), o), device_id_type=MESH,
        )

    def left_copy(g, d):
        to = lax.rem(z + d, nz)
        return pltpu.make_async_remote_copy(
            src_ref=mine.at[g], dst_ref=left.at[g, y, qh, a],
            send_sem=l_send.at[g, d], recv_sem=l_recv.at[g, qh, a],
            device_id=(band_of, 2 * to + y), device_id_type=MESH,
        )

    def y_copy(g):
        return pltpu.make_async_remote_copy(
            src_ref=left.at[g, y], dst_ref=left.at[g, y],
            send_sem=y_send.at[g], recv_sem=y_recv.at[g],
            device_id=(a, partner), device_id_type=MESH,
        )

    def finish_sums(g):
        for d in range(1, nz):
            a2_copy(g, d).wait()
        acc = part2[g, z].astype(F32)
        for d in range(1, nz):
            acc = acc + recv2[g, d - 1].astype(F32)
        done = acc.astype(BF16)
        mine[g] = done
        for d in range(1, nz):
            left_copy(g, d).start()

        @pl.when(jnp.logical_not(home))
        def _():
            left_copy(g, 0).start()

        for e in range(1, n_aux):
            right_copy(g, e).start()
        right[g, a] = done

        @pl.when(home)
        def _():
            left[g, y, qh, a] = done

    def pass_on(g):
        for s in range(n_aux):
            for q in range(hr):
                @pl.when(jnp.logical_not(jnp.logical_and(s == a, a * ratio + 2 * q + y == o)))
                def _():
                    pltpu.make_async_remote_copy(
                        src_ref=mine.at[g], dst_ref=left.at[g, y, q, s],
                        send_sem=l_send.at[g, 0], recv_sem=l_recv.at[g, q, s],
                        device_id=(band_of, lax.rem(o + 1, n_ao)), device_id_type=MESH,
                    ).wait_recv()
        y_copy(g).start()

    def last_waits(g):
        for d in range(1, nz):
            left_copy(g, d).wait_send()

        @pl.when(jnp.logical_not(home))
        def _():
            left_copy(g, 0).wait_send()

        for e in range(1, n_aux):
            right_copy(g, e).wait()
        y_copy(g).wait()

    first_groups = max(1, n_groups // 2)
    rows_of_group(0)
    for d in range(1, reach + 1):
        share_copy(d).wait()
        for e in range(1, n_aux):
            forward_copy(d, e).start()
    for g in range(1, first_groups):
        rows_of_group(g)
    for d in range(1, reach + 1):
        for e in range(1, n_aux):
            forward_copy(d, e).wait()
    ready = first_groups
    for step in range(n_groups + 4):
        if step < n_groups:
            if step >= ready:
                rows_of_group(step)
            pairs_of_group(step)
        if 0 <= step - 1 < n_groups:
            second_level(step - 1)
        if 0 <= step - 2 < n_groups:
            finish_sums(step - 2)
        if 0 <= step - 3 < n_groups:
            pass_on(step - 3)
    for g in range(n_groups):
        last_waits(g)


def integrals_kernel(left, right, out, wide, left_f, right_f):
    n_groups, parities, hr, n_aux, gv, width, active = left.shape
    nvec = n_groups * n_aux * gv
    per_step = out.shape[0] // active

    @pl.when(pl.program_id(0) == 0)
    def _():
        right_f[...] = right[...].reshape(nvec, width, active).astype(F32)
        for i in range(width):
            wide[:, pl.ds(i * active, active)] = right_f[:, i, :].astype(BF16)
        for q in range(parities * hr):
            value = left[:, q % 2, q // 2].reshape(nvec, width, active).astype(F32)
            left_f[q] = value

    k = pl.program_id(0) * per_step
    q, i = k // width, lax.rem(k, width)
    tall = jnp.concatenate(
        [left_f[q, :, i + s, :].astype(BF16) for s in range(per_step)], axis=1
    )
    out[...] = lax.dot_general(
        tall, wide[...], (((0,), (0,)), ((), ())), preferred_element_type=F32
    )


def on_device(n_aux, n_ao, cholesky, coeffs):
    nvec, rows, basis = cholesky.shape
    active = coeffs.shape[1]
    width, band = active // n_ao, active // n_aux
    ratio = n_ao // n_aux
    nz = n_ao // 2
    reach = n_ao // 2
    n_groups = 4 if nvec % 4 == 0 else 1
    gv = nvec // n_groups
    deep = (reach + 1) * rows
    dma = pltpu.SemaphoreType.DMA
    vmem = pl.BlockSpec(memory_space=pltpu.VMEM)
    left_shape = (n_groups, 2, ratio // 2, n_aux, gv, width, active)
    right_shape = (n_groups, n_aux, gv, width, active)
    left, right = pl.pallas_call(
        functools.partial(pairs_kernel, n_aux, n_ao, n_groups),
        out_shape=(
            jax.ShapeDtypeStruct(left_shape, BF16),
            jax.ShapeDtypeStruct(right_shape, BF16),
        ),
        in_specs=[pl.BlockSpec(memory_space=pl.ANY), vmem],
        out_specs=(vmem, vmem),
        scratch_shapes=[
            pltpu.VMEM((nvec, rows, deep), BF16),
            pltpu.VMEM((deep, active), BF16),
            pltpu.VMEM((active, rows), BF16),
            pltpu.VMEM((active, rows), BF16),
            pltpu.VMEM((active, rows), BF16),
            pltpu.VMEM((nvec * active, deep), BF16),
            pltpu.VMEM((n_groups, 2, nz, gv, width, active), BF16),
            pltpu.VMEM((n_groups, nz, gv, width, active), BF16),
            pltpu.VMEM((n_groups, nz, gv, width, active), BF16),
            pltpu.VMEM((n_groups, nz - 1, gv, width, active), BF16),
            pltpu.VMEM((n_groups, gv, width, active), BF16),
            dma((nvec,)),
            dma((reach,)),
            dma((reach,)),
            dma((reach, n_aux - 1)),
            dma((reach, n_aux - 1)),
            dma((n_groups,)),
            dma((n_groups,)),
            dma((n_groups, nz - 1)),
            dma((n_groups, nz - 1)),
            dma((n_groups, n_aux - 1)),
            dma((n_groups, n_aux - 1)),
            dma((n_groups, nz)),
            dma((n_groups, ratio // 2, n_aux)),
            dma((n_groups,)),
            dma((n_groups,)),
        ],
        compiler_params=pltpu.CompilerParams(
            has_side_effects=True, vmem_limit_bytes=62 << 20
        ),
    )(cholesky, coeffs)
    per_step = 4
    whole = lambda *shape: pl.BlockSpec(shape, lambda k: (0,) * len(shape))
    return pl.pallas_call(
        integrals_kernel,
        grid=(band // per_step,),
        out_shape=jax.ShapeDtypeStruct((band * active, width * active), F32),
        in_specs=[whole(*left_shape), whole(*right_shape)],
        out_specs=pl.BlockSpec((per_step * active, width * active), lambda k: (k, 0)),
        scratch_shapes=[
            pltpu.VMEM((n_aux * nvec, width * active), BF16),
            pltpu.VMEM((ratio, n_aux * nvec, width, active), F32),
            pltpu.VMEM((n_aux * nvec, width, active), F32),
        ],
    )(left, right)


def solution(mesh):
    return jax.shard_map(
        functools.partial(on_device, mesh.shape["aux"], mesh.shape["ao"]),
        mesh=mesh,
        in_specs=(P("aux", "ao", None), P("ao", None)),
        out_specs=P("aux", "ao"),
        check_vma=False,
    )
```
